256 devices in a mesh: parts: 4 (over x, y), pts: 64 (over z, core).
Axes of the slice: x: 2, y: 2, z: 32, core: 2. Of those that a mesh axis runs over, the one named last changes fastest.
The devices are a block of a 4x8x32 slice.
Arguments:
- grid_weights: float32 [512, 128, 128], P(('parts', 'pts')), parts along dimension 0, may hold values from -6 to 6
- direction: float32 [512, 128, 128], P(('parts', 'pts')), parts along dimension 0, may hold values from -6 to 6
- kern_x: float32 [128, 128], replicated
- kern_y: float32 [128, 128], replicated
- kern_z: float32 [128, 128], replicated
- interp: bfloat16 [32768, 128, 256], P(('parts', 'pts')), parts along dimension 0, may hold values from -4 to 4
- block_corner: int32 [3, 32768], P(None, ('parts', 'pts')), parts along dimension 1, may hold values from 0 to 120, as said below
- block_offsets: int32 [32768, 256], P(('parts', 'pts')), parts along dimension 0, may hold values from 0 to 2047, as said below
- labels: int32 [32768, 128], P(('parts', 'pts')), parts along dimension 0, may hold values 0 or 1
- trial_steps: float32 [5], replicated, may hold values from 0.05 to 2
- accept: int32 [1], replicated, may hold values from 0 to 4
Outputs:
- new_weights: float32 [512, 128, 128], P(('parts', 'pts')), parts along dimension 0
- grid_gradient: float32 [512, 128, 128], P(('parts', 'pts')), parts along dimension 0
- curvature: float32 [32768, 128], P(('parts', 'pts')), parts along dimension 0
- trial_objective: float32 [20], P('parts'), parts along dimension 0
- trial_slope: float32 [20], P('parts'), parts along dimension 0
The draws below stay inside these ranges and needn't reach their ends.
There are 4 independent parts, one for each index of `parts`. The reference program is written for one: setup_inputs(seed, part) draws one part's arguments, and reference() takes and returns one part's arrays. A program takes and returns all parts, laid end to end along the dimension named above; an argument that names none is the same for every part. Nothing has to cross between parts.
Inputs may be any that keep to these rules, and one draw needn't show every extreme that they name: `block_corner`: row 0 lies in 0 to 112, row 1 in 0 to 112, row 2 in 0 to 120. `block_offsets`: the 256 offsets of one block are distinct.
All inputs are finite; a program needn't handle non-finite values. No bound on the sum of `labels` on one device may be relied on, other than what follows from the above.
Results may differ from the reference program's by a relative error of at most 0.0075.
The reference program's roundings to bfloat16 on the way count: a program that leaves them out, or rounds other values in their place, can miss the bound.
Values may be sent and summed in bfloat16 or wider, within the bound.
No kernel may reach another device: no remote copies, remote signals or barrier semaphores. Data moves between devices by JAX's collectives and lax.ppermute only.
A program may use at most 128 MiB of HBM per device.

```python
import math
import jax
import jax.numpy as jnp
from jax import lax

GX = 128
GY = 128
GZ = 128
BOXX = 16
BOXY = 16
BOXZ = 8
COLS = 256
PTS_BLOCK = 128
NTRIAL = 5
NB = 128
BLOCKS = 8192
POINTS = 1048576
N_PTS = 64


def kernel_table(key, size, salt):
    key = jax.random.fold_in(key, salt)
    key_len, key_noise, key_gain = jax.random.split(key, 3)
    length = jax.random.uniform(key_len, (), jnp.float32, 4.0, 16.0)
    noise_scale = 0.15
    position = jnp.arange(size, dtype=jnp.float32)
    spacing = jnp.abs(position[:, None] - position[None, :])
    smooth = jnp.exp(-spacing / length)
    noise = jax.random.normal(key_noise, (size, size), jnp.float32)
    symmetric = (noise + noise.T) * 0.7071
    gains = jax.random.uniform(key_gain, (size,), jnp.float32, 0.7, 1.4)
    table = gains[:, None] * (smooth + noise_scale * symmetric) * gains[None, :] / jnp.sqrt(length)
    return table.astype(jnp.float32)


def draw_kern_x(key, part):
    return kernel_table(key, GX, 11)


def draw_kern_y(key, part):
    return kernel_table(key, GY, 23)


def draw_kern_z(key, part):
    return kernel_table(key, GZ, 37)


def draw_interp(key, part):
    key = jax.random.fold_in(key, 53)
    ratio = 6.0
    base = jnp.clip(jax.random.normal(key, (BLOCKS, PTS_BLOCK, COLS), jnp.float32), -4.0, 4.0)
    level = jnp.arange(BLOCKS, dtype=jnp.float32) / max(BLOCKS - 1, 1)
    scale = jnp.exp(jnp.log(ratio) * level) / jnp.sqrt(ratio)
    table = base * scale[:, None, None] / jnp.sqrt(jnp.float32(COLS))
    return jnp.clip(table, -4.0, 4.0).astype(jnp.bfloat16)


def draw_block_corner(key, part):
    limits = jnp.array([GX - BOXX, GY - BOXY, GZ - BOXZ], jnp.int32)
    corner = jax.random.randint(key, (3, BLOCKS), 0, limits[:, None] + 1)
    corner = corner.at[:, 0].set(limits)
    corner = corner.at[:, BLOCKS - 1].set(0)
    return corner.astype(jnp.int32)


def draw_block_offsets(key, part):
    keys = jax.random.split(key, BLOCKS)

    def choose_cells(one_key):
        return jax.random.permutation(one_key, BOXX * BOXY * BOXZ)[:COLS]
    return jax.vmap(choose_cells)(keys).astype(jnp.int32)


def place_ends(values, rng, smallest, top_value):
    longest = values.shape.index(max(values.shape))
    spots = []
    for shift in (0, 1):
        where = [jax.random.randint(jax.random.fold_in(rng, axis), (), 0, length) for axis, length in enumerate(values.shape)]
        where[longest] = (where[longest] + shift) % values.shape[longest]
        spots.append(tuple(where))
    return values.at[spots[0]].set(smallest).at[spots[1]].set(top_value)


def levels(rng, shape, pieces, smallest, top_value):
    def one(dim, blocks):
        steps = jax.random.uniform(jax.random.fold_in(jax.random.fold_in(rng, 6), dim), (blocks,), jnp.float32, smallest / len(pieces), top_value / len(pieces))
        return jnp.repeat(jnp.exp(steps), shape[dim] // blocks).reshape((-1,) + (1,) * (len(shape) - dim - 1))

    level = one(*pieces[0])
    for cut in pieces[1:]:
        level = level * one(*cut)
    return level


def bell_draw(rng, dims, width, limit, shards=(), held_as=jnp.bfloat16):
    values = width * jax.random.normal(rng, dims, jnp.float32)
    if shards:
        values = values * levels(rng, dims, shards, -0.22, 0.18)
    return jnp.clip(values, -limit, limit).astype(held_as)


def setup_inputs(seed: int = 0, part: int = 0) -> dict:
    key_list = jax.random.split(jax.random.key(seed), 12)
    own_keys = jax.random.split(jax.random.fold_in(key_list[11], part), 12)
    grid_weights = bell_draw(own_keys[0], (GX, GY, GZ), 1.0, 6.0, ((0, 64),), jnp.float32)
    direction = bell_draw(own_keys[1], (GX, GY, GZ), 1.0, 6.0, ((0, 64),), jnp.float32)
    kern_x = draw_kern_x(jax.random.fold_in(key_list[11], 71), part)
    kern_y = draw_kern_y(jax.random.fold_in(key_list[11], 71), part)
    kern_z = draw_kern_z(jax.random.fold_in(key_list[11], 71), part)
    interp = draw_interp(jax.random.fold_in(jax.random.fold_in(key_list[11], part), 71), part)
    block_corner = draw_block_corner(jax.random.fold_in(jax.random.fold_in(key_list[11], part), 71), part)
    block_offsets = draw_block_offsets(jax.random.fold_in(jax.random.fold_in(key_list[11], part), 71), part)
    labels = place_ends((jax.random.randint(own_keys[8], (BLOCKS, PTS_BLOCK), 0, 2) < 1).astype(jnp.int32), jax.random.fold_in(own_keys[8], 1), 0, 1)
    trial_steps = jnp.clip(jnp.exp(jax.random.uniform(key_list[9], (NTRIAL,), jnp.float32, math.log(0.05), math.log(2.0))), 0.05, 2.0)
    accept = jax.random.randint(key_list[10], (1,), 0, NTRIAL).astype(jnp.int32)
    return dict(grid_weights=grid_weights, direction=direction, kern_x=kern_x, kern_y=kern_y, kern_z=kern_z, interp=interp, block_corner=block_corner, block_offsets=block_offsets, labels=labels, trial_steps=trial_steps, accept=accept)


HIGHEST = lax.Precision.HIGHEST


def plane_mix(fields, kern_y, kern_z):
    inner_mix = jnp.einsum('...bc,zc->...bz', fields, kern_z, precision=HIGHEST)
    return jnp.einsum('...xbz,yb->...xyz', inner_mix, kern_y, precision=HIGHEST).astype(jnp.bfloat16)


def depth_mix(partial_value, kern_x):
    return jnp.einsum('xa,...ayz->...xyz', kern_x, partial_value.astype(jnp.float32), precision=HIGHEST)


def cell_ids_of(block_corner, block_offsets):
    plane_off = block_offsets // (BOXY * BOXZ)
    row_off = (block_offsets // BOXZ) % BOXY
    depth_off = block_offsets % BOXZ
    cell_x = block_corner[0][:, None] + plane_off
    cell_y = block_corner[1][:, None] + row_off
    cell_z = block_corner[2][:, None] + depth_off
    return ((cell_x * GY + cell_y) * GZ + cell_z).astype(jnp.int32)


def interpolate(interp, values):
    count_fields = values.shape[0]
    groups = interp.reshape(N_PTS, NB, PTS_BLOCK, COLS)
    grouped = jnp.moveaxis(values.reshape(count_fields, N_PTS, NB, COLS), 1, 0)

    def one_group(operands):
        return jnp.einsum('bpc,fbc->fbp', operands[0].astype(jnp.float32), operands[1].astype(jnp.float32), precision=HIGHEST)

    result = lax.map(one_group, (groups, grouped))
    return jnp.moveaxis(result, 0, 1).reshape(count_fields, N_PTS * NB, PTS_BLOCK)


def column_terms(interp, residual):
    groups = interp.reshape(N_PTS, NB, PTS_BLOCK, COLS)
    grouped = residual.reshape(N_PTS, NB, PTS_BLOCK)

    def one_group(operands):
        return jnp.einsum('bpc,bp->bc', operands[0].astype(jnp.float32), operands[1].astype(jnp.float32), precision=HIGHEST)

    return lax.map(one_group, (groups, grouped)).reshape(N_PTS * NB, COLS)


def reference(grid_weights, direction, kern_x, kern_y, kern_z, interp, block_corner, block_offsets, labels, trial_steps, accept):
    fields = jnp.stack([grid_weights, direction])
    mixed_grid = depth_mix(plane_mix(fields, kern_y, kern_z), kern_x)
    quad_gu = jnp.sum(grid_weights * mixed_grid[0])
    quad_du = jnp.sum(direction * mixed_grid[0])
    quad_dv = jnp.sum(direction * mixed_grid[1])
    cell_ids = cell_ids_of(block_corner, block_offsets)
    flat_grid = mixed_grid.astype(jnp.bfloat16).reshape(2, -1)
    values = jnp.take(flat_grid, cell_ids, axis=1)
    latent_pair = interpolate(interp, values)
    latent = latent_pair[0]
    slope_pt = latent_pair[1]
    target = labels.astype(jnp.float32)
    signed = 2.0 * target - 1.0
    trial_latent = latent[None] + trial_steps[:, None, None] * slope_pt[None]
    loglik = jnp.sum(jax.nn.log_sigmoid(signed[None] * trial_latent), axis=(1, 2))
    descent = jnp.sum((target[None] - jax.nn.sigmoid(trial_latent)) * slope_pt[None], axis=(1, 2))
    prior = 0.5 * (quad_gu + 2.0 * trial_steps * quad_du + trial_steps * trial_steps * quad_dv)
    trial_objective = (loglik - prior) / POINTS
    trial_slope = (descent - quad_du - trial_steps * quad_dv) / POINTS
    chosen = jnp.sum(jnp.where(jnp.arange(NTRIAL) == accept[0], trial_steps, 0.0))
    probability = jax.nn.sigmoid(latent + chosen * slope_pt)
    residual = (target - probability).astype(jnp.bfloat16)
    column_term = column_terms(interp, residual)
    spread = jnp.zeros((GX * GY * GZ,), jnp.float32).at[cell_ids.reshape(-1)].add(column_term.reshape(-1)).reshape(GX, GY, GZ)
    new_weights = grid_weights + chosen * direction
    grid_gradient = spread - new_weights
    bend_grid = depth_mix(plane_mix(grid_gradient[None], kern_y, kern_z), kern_x)
    bend_values = jnp.take(bend_grid.astype(jnp.bfloat16).reshape(1, -1), cell_ids, axis=1)
    bend_pt = interpolate(interp, bend_values)[0]
    curvature = probability * (1.0 - probability) * bend_pt
    return new_weights, grid_gradient, curvature, trial_objective, trial_slope
```

```python
import jax
import jax.numpy as jnp
from jax import lax
from jax.experimental import pallas as pl
from jax.experimental.pallas import tpu as pltpu
from jax.sharding import Mesh
from jax.sharding import PartitionSpec as P

BOXX = 16
BOXY = 16
BOXZ = 8
NTRIAL = 5
CORES = 2
GROUP = 8
LOADS = 16
FLUSHES = 16
PTS = ("pts_0", "pts_1")
PARTS_PTS = ("parts", "pts_0", "pts_1")

HIGHEST = lax.Precision.HIGHEST
F32 = jnp.float32
BF16 = jnp.bfloat16
I32 = jnp.int32


def plane_mix(fields, kern_y, kern_z):
    inner_mix = jnp.einsum("...bc,zc->...bz", fields, kern_z, precision=HIGHEST)
    return jnp.einsum("...xbz,yb->...xyz", inner_mix, kern_y, precision=HIGHEST).astype(BF16)


def kron_rows(fields, kern_x, kern_y, kern_z, staged):
    count, slab, size_y, size_z = fields.shape
    devices = lax.axis_size(PTS)
    cores = lax.axis_size("pts_1")
    planes = plane_mix(fields, kern_y, kern_z)
    if staged:
        sent = planes.reshape(count, slab, cores, devices // cores, size_y // devices, size_z)
        sent = sent.transpose(3, 2, 0, 1, 4, 5).reshape(devices, count, slab, -1, size_z)
    else:
        sent = planes.reshape(count, slab, devices, size_y // devices, size_z)
        sent = sent.transpose(2, 0, 1, 3, 4)
    got = lax.all_to_all(sent, PTS, 0, 0, tiled=True)
    lines = got.transpose(1, 3, 0, 2, 4).reshape(count, size_y // devices, -1, size_z)
    mixed = jnp.einsum("xa,fyaz->fyxz", kern_x, lines.astype(F32), precision=HIGHEST)
    low = mixed.astype(BF16)
    if staged:
        whole = lax.all_gather(low, "pts_0", axis=0)
        whole = lax.all_gather(whole, "pts_1", axis=0)
        return whole.reshape(devices, *low.shape)
    return lax.all_gather(low, PTS, axis=0)


def depth_lines(corner_z, offsets, size_z):
    line = lax.broadcasted_iota(I32, (size_z, offsets.shape[1]), 0)
    return line == corner_z + (offsets & (BOXZ - 1))


def load_rows(grid_ref, chunk, step):
    devices, count, slab = chunk.shape[:3]
    for d in range(devices):
        for f in range(count):
            for r in range(slab):
                row = (step * devices + d) * slab + r
                grid_ref[f, row] = chunk[d, f, r].astype(F32)


def box_values(grid_ref, corner_ref, block, offsets, depth_mask):
    columns = offsets.shape[1]
    size_z = grid_ref.shape[-1]
    row = ((offsets // BOXZ) & (BOXY - 1)) * BOXX + offsets // (BOXY * BOXZ)
    wanted = lax.broadcasted_iota(I32, (BOXX * BOXY, columns), 0) == row
    pick = jnp.where(depth_mask, 1.0, 0.0).astype(BF16)
    found = []
    for f in range(grid_ref.shape[0]):
        box = grid_ref[f, pl.ds(corner_ref[1, block], BOXY), pl.ds(corner_ref[0, block], BOXX), :]
        box = box.reshape(BOXY * BOXX, size_z).astype(BF16)
        taken = jnp.dot(box, pick, preferred_element_type=F32)
        found.append(jnp.sum(jnp.where(wanted, taken, 0.0), axis=0, keepdims=True))
    return jnp.concatenate(found, axis=0).astype(BF16) if len(found) > 1 else found[0].astype(BF16)


def on_points(values, interp):
    return lax.dot_general(values, interp, (((1,), (1,)), ((), ())), preferred_element_type=F32)


def forward_kernel(
    corner_ref,
    core_ref,
    chosen_ref,
    rows_ref,
    interp_ref,
    offsets_ref,
    labels_ref,
    latent_ref,
    slope_ref,
    own_ref,
    other_ref,
    grid_ref,
    sum_ref,
):
    step = pl.program_id(0)
    steps = pl.num_programs(0)
    size_x = sum_ref.shape[0]
    size_z = sum_ref.shape[-1]

    @pl.when(step < LOADS)
    def _():
        load_rows(grid_ref, rows_ref, step)
        some = size_x // LOADS
        sum_ref[pl.ds(step * some, some)] = jnp.zeros((some, *sum_ref.shape[1:]), F32)

    @pl.when((step >= LOADS) & (step < steps - FLUSHES))
    def _():
        first = (step - LOADS) * GROUP
        masks = []
        points = []
        for k in range(GROUP):
            offsets = offsets_ref[k : k + 1, :]
            mask = depth_lines(corner_ref[2, first + k], offsets, size_z)
            values = box_values(grid_ref, corner_ref, first + k, offsets, mask)
            points.append(on_points(values, interp_ref[k]))
        latent = jnp.concatenate([p[0:1] for p in points], axis=0)
        slope = jnp.concatenate([p[1:2] for p in points], axis=0)
        latent_ref[...] = latent
        slope_ref[...] = slope
        probability = 1.0 / (1.0 + jnp.exp(-(latent + chosen_ref[0] * slope)))
        residual = labels_ref[...].astype(F32) - probability
        for k in range(GROUP):
            offsets = offsets_ref[k : k + 1, :]
            mask = depth_lines(corner_ref[2, first + k], offsets, size_z)
            term = jnp.dot(
                residual[k : k + 1].astype(BF16), interp_ref[k], preferred_element_type=F32
            )
            high = term.astype(BF16).astype(F32)
            low = term - high
            placed = jnp.concatenate(
                [
                    jnp.where(mask, high, 0.0).astype(BF16),
                    jnp.where(mask, low, 0.0).astype(BF16),
                ],
                axis=0,
            )
            row = lax.broadcasted_iota(I32, (BOXX * BOXY, offsets.shape[1]), 0)
            hot = jnp.where(row == offsets // BOXZ, 1.0, 0.0).astype(BF16)
            added = lax.dot_general(
                hot, placed, (((1,), (1,)), ((), ())), preferred_element_type=F32
            )
            added = (added[:, :size_z] + added[:, size_z:]).reshape(BOXX, BOXY, size_z)
            spot = (
                pl.ds(corner_ref[0, first + k], BOXX),
                pl.ds(corner_ref[1, first + k], BOXY),
                slice(None),
            )
            sum_ref[spot] = sum_ref[spot] + added

    half = FLUSHES // CORES
    for part, (spread_ref, core) in enumerate(
        ((other_ref, CORES - 1 - core_ref[0]), (own_ref, core_ref[0]))
    ):
        start = steps - FLUSHES + part * half

        @pl.when((step >= start) & (step < start + half))
        def _():
            chips, slab = spread_ref.shape[:2]
            for c in range(chips):
                for r in range(slab):
                    device = ((step - start) * chips + c) * CORES + core
                    spread_ref[c, r] = sum_ref[device * slab + r]


def bend_kernel(
    corner_ref,
    chosen_ref,
    rows_ref,
    interp_ref,
    offsets_ref,
    latent_ref,
    slope_ref,
    curvature_ref,
    grid_ref,
):
    step = pl.program_id(0)
    size_z = grid_ref.shape[-1]

    @pl.when(step < LOADS)
    def _():
        load_rows(grid_ref, rows_ref, step)

    @pl.when(step >= LOADS)
    def _():
        first = (step - LOADS) * GROUP
        points = []
        for k in range(GROUP):
            offsets = offsets_ref[k : k + 1, :]
            mask = depth_lines(corner_ref[2, first + k], offsets, size_z)
            values = box_values(grid_ref, corner_ref, first + k, offsets, mask)
            points.append(on_points(values, interp_ref[k]))
        bend = jnp.concatenate(points, axis=0)
        probability = 1.0 / (1.0 + jnp.exp(-(latent_ref[...] + chosen_ref[0] * slope_ref[...])))
        curvature_ref[...] = probability * (1.0 - probability) * bend


def run_forward(corner, core, chosen, rows, interp, offsets, labels):
    devices, count, slab, size_x, size_z = rows.shape
    blocks, points, columns = interp.shape
    groups = blocks // GROUP
    load = devices // LOADS
    at = lambda i: jnp.clip(i - LOADS, 0, groups - 1)
    chips = devices // CORES
    half = FLUSHES // CORES
    flush = lambda i, part: (jnp.clip(i - LOADS - groups - part * half, 0, half - 1), 0, 0, 0)
    flush_block = (chips // half, size_x // devices, devices * slab, size_z)
    flushed = jax.ShapeDtypeStruct((chips, *flush_block[1:]), F32)
    point_spec = pl.BlockSpec((GROUP, points), lambda i, *_: (at(i), 0))
    return pl.pallas_call(
        forward_kernel,
        grid_spec=pltpu.PrefetchScalarGridSpec(
            num_scalar_prefetch=3,
            grid=(LOADS + groups + FLUSHES,),
            in_specs=[
                pl.BlockSpec(
                    (load, count, slab, size_x, size_z),
                    lambda i, *_: (jnp.minimum(i, LOADS - 1), 0, 0, 0, 0),
                ),
                pl.BlockSpec((GROUP, points, columns), lambda i, *_: (at(i), 0, 0)),
                pl.BlockSpec((GROUP, columns), lambda i, *_: (at(i), 0)),
                point_spec,
            ],
            out_specs=[
                point_spec,
                point_spec,
                pl.BlockSpec(flush_block, lambda i, *_: flush(i, 1)),
                pl.BlockSpec(flush_block, lambda i, *_: flush(i, 0)),
            ],
            scratch_shapes=[
                pltpu.VMEM((count, devices * slab, size_x, size_z), F32),
                pltpu.VMEM((size_x, devices * slab, size_z), F32),
            ],
        ),
        out_shape=[
            jax.ShapeDtypeStruct((blocks, points), F32),
            jax.ShapeDtypeStruct((blocks, points), F32),
            flushed,
            flushed,
        ],
        name="forward",
    )(corner, core, chosen, rows, interp, offsets, labels)


def run_bend(corner, chosen, rows, interp, offsets, latent, slope):
    devices, count, slab, size_x, size_z = rows.shape
    blocks, points, columns = interp.shape
    groups = blocks // GROUP
    at = lambda i: jnp.maximum(i - LOADS, 0)
    point_spec = pl.BlockSpec((GROUP, points), lambda i, *_: (at(i), 0))
    return pl.pallas_call(
        bend_kernel,
        grid_spec=pltpu.PrefetchScalarGridSpec(
            num_scalar_prefetch=2,
            grid=(LOADS + groups,),
            in_specs=[
                pl.BlockSpec(
                    (devices // LOADS, count, slab, size_x, size_z),
                    lambda i, *_: (jnp.minimum(i, LOADS - 1), 0, 0, 0, 0),
                ),
                pl.BlockSpec((GROUP, points, columns), lambda i, *_: (at(i), 0, 0)),
                pl.BlockSpec((GROUP, columns), lambda i, *_: (at(i), 0)),
                point_spec,
                point_spec,
            ],
            out_specs=point_spec,
            scratch_shapes=[pltpu.VMEM((count, devices * slab, size_x, size_z), F32)],
        ),
        out_shape=jax.ShapeDtypeStruct((blocks, points), F32),
        name="bend",
    )(corner, chosen, rows, interp, offsets, latent, slope)


def body(
    grid_weights,
    direction,
    kern_x,
    kern_y,
    kern_z,
    interp,
    block_corner,
    block_offsets,
    labels,
    trial_steps,
    accept,
):
    slab, size_y, size_z = grid_weights.shape
    devices = lax.axis_size(PTS)
    points = interp.shape[0] * interp.shape[1] * devices
    chosen = jnp.sum(jnp.where(jnp.arange(NTRIAL) == accept[0], trial_steps, 0.0))
    fields = jnp.stack([grid_weights, direction])
    rows = kron_rows(fields, kern_x, kern_y, kern_z, True)
    core = lax.axis_index("pts_1")
    latent, slope_pt, own, other = run_forward(
        block_corner, core[None], chosen[None], rows, interp, block_offsets, labels
    )
    swap = [(c, CORES - 1 - c) for c in range(CORES)]
    part = (own + lax.ppermute(other, "pts_1", swap)).astype(BF16)
    spread = lax.psum_scatter(part, "pts_0", scatter_dimension=0, tiled=True)[0].astype(F32)

    mine = lax.dynamic_slice_in_dim(rows, lax.axis_index(PTS) * slab, slab, 3).astype(F32)
    weights = jnp.stack([grid_weights, direction]).reshape(2, slab, devices, -1, size_z)
    quad = jnp.einsum("gxdyz,dfyxz->gf", weights, mine, precision=HIGHEST)
    target = labels.astype(F32)
    signed = 2.0 * target - 1.0
    trial_latent = latent[None] + trial_steps[:, None, None] * slope_pt[None]
    loglik = jnp.sum(jax.nn.log_sigmoid(signed[None] * trial_latent), axis=(1, 2))
    descent = jnp.sum((target[None] - jax.nn.sigmoid(trial_latent)) * slope_pt[None], axis=(1, 2))
    sums = lax.psum(jnp.concatenate([loglik, descent, quad.reshape(-1)]), PTS)
    loglik = sums[:NTRIAL]
    descent = sums[NTRIAL : 2 * NTRIAL]
    quad_gu, quad_du, quad_dv = sums[2 * NTRIAL], sums[2 * NTRIAL + 2], sums[2 * NTRIAL + 3]
    prior = 0.5 * (quad_gu + 2.0 * trial_steps * quad_du + trial_steps * trial_steps * quad_dv)
    trial_objective = (loglik - prior) / points
    trial_slope = (descent - quad_du - trial_steps * quad_dv) / points

    new_weights = grid_weights + chosen * direction
    grid_gradient = spread - new_weights
    bend_rows = kron_rows(grid_gradient[None], kern_x, kern_y, kern_z, False)
    curvature = run_bend(
        block_corner, chosen[None], bend_rows, interp, block_offsets, latent, slope_pt
    )
    return (new_weights, grid_gradient, curvature, trial_objective, trial_slope)


def solution(mesh):
    parts = mesh.shape["parts"]
    finer = Mesh(mesh.devices.reshape(parts, -1, CORES), ("parts", "pts_0", "pts_1"))
    placed = (
        P(PARTS_PTS, None, None),
        P(PARTS_PTS, None, None),
        P(),
        P(),
        P(),
        P(PARTS_PTS, None, None),
        P(None, PARTS_PTS),
        P(PARTS_PTS, None),
        P(PARTS_PTS, None),
        P(),
        P(),
    )
    return jax.shard_map(
        body,
        mesh=finer,
        in_specs=placed,
        out_specs=(
            P(PARTS_PTS, None, None),
            P(PARTS_PTS, None, None),
            P(PARTS_PTS, None),
            P("parts"),
            P("parts"),
        ),
        check_vma=False,
    )
```

```python
import jax
import jax.numpy as jnp
from jax import lax
from jax.experimental import pallas as pl
from jax.experimental.pallas import tpu as pltpu
from jax.sharding import Mesh
from jax.sharding import PartitionSpec as P

BOXX = 16
BOXY = 16
BOXZ = 8
NTRIAL = 5
CORES = 2
GROUP = 8
LOADS = 16
FLUSHES = 16
MIXES = 16
PTS = ("pts_0", "pts_1")
PARTS_PTS = ("parts", "pts_0", "pts_1")

HIGHEST = lax.Precision.HIGHEST
F32 = jnp.float32
BF16 = jnp.bfloat16
I32 = jnp.int32


def plane_mix(fields, kern_y, kern_z):
    inner_mix = jnp.einsum("...bc,zc->...bz", fields, kern_z, precision=HIGHEST)
    return jnp.einsum("...xbz,yb->...xyz", inner_mix, kern_y, precision=HIGHEST).astype(BF16)


def pieces_of(array):
    high = lax.reduce_precision(array, 8, 7)
    rest = array - high
    middle = lax.reduce_precision(rest, 8, 7)
    return high.astype(BF16), middle.astype(BF16), (rest - middle).astype(BF16)


def depth_lines(corner_z, offsets, size_z):
    line = lax.broadcasted_iota(I32, (size_z, offsets.shape[1]), 0)
    return line == corner_z + (offsets & (BOXZ - 1))


def load_planes(plane_ref, chunk, step, slab_rows):
    devices = chunk.shape[0]
    for d in range(devices):
        first = pl.multiple_of((step * devices + d) * slab_rows, slab_rows)
        plane_ref[pl.ds(first, slab_rows), :] = chunk[d, :slab_rows].astype(F32)


def mix_planes(grid_ref, plane_ref, kern, step, size_x, size_y):
    some = size_y // MIXES
    size_z = grid_ref.shape[-1]
    for k in range(0, some, 2):
        row = step * some + k
        pair = [plane_ref[pl.ds(row + r, size_x, stride=size_y), :].astype(BF16) for r in range(2)]
        mixed = jnp.dot(kern, jnp.concatenate(pair, axis=1), preferred_element_type=F32)
        mixed = mixed[:size_x] + mixed[size_x : 2 * size_x] + mixed[2 * size_x :]
        for r in range(2):
            first = pl.multiple_of((row + r) * size_x, size_x)
            grid_ref[pl.ds(first, size_x), :] = mixed[:, r * size_z : (r + 1) * size_z]


def prepare(step, kern_ref, rows_ref, plane_ref, grid_ref):
    size_x = kern_ref.shape[1]
    size_y = plane_ref.shape[0] // size_x
    slab_rows = plane_ref.shape[0] // (LOADS * rows_ref.shape[0])

    @pl.when(step < LOADS)
    def _():
        load_planes(plane_ref, rows_ref, step, slab_rows)

    @pl.when((step >= LOADS) & (step < LOADS + MIXES))
    def _():
        mix_planes(grid_ref, plane_ref, kern_ref[...], step - LOADS, size_x, size_y)


def own_planes(image_ref, grid_ref, device, size_x):
    slab, size_y = image_ref.shape[:2]
    for r in range(slab):
        image_ref[r] = grid_ref[pl.ds(device * slab + r, size_y, stride=size_x), :]


def box_values(grid_ref, corner_ref, block, offsets, depth_mask, size_x):
    row = ((offsets // BOXZ) & (BOXY - 1)) * BOXX + offsets // (BOXY * BOXZ)
    wanted = lax.broadcasted_iota(I32, (BOXX * BOXY, offsets.shape[1]), 0) == row
    pick = jnp.where(depth_mask, 1.0, 0.0).astype(BF16)
    first = corner_ref[1, block] * size_x + corner_ref[0, block]
    box = [grid_ref[pl.ds(first + k * size_x, BOXX), :].astype(BF16) for k in range(BOXY)]
    taken = jnp.dot(jnp.concatenate(box, axis=0), pick, preferred_element_type=F32)
    return jnp.sum(jnp.where(wanted, taken, 0.0), axis=0, keepdims=True).astype(BF16)


def on_points(values, interp):
    return lax.dot_general(values, interp, (((1,), (1,)), ((), ())), preferred_element_type=F32)


def field_points(first, corner_ref, offsets_ref, interp_ref, grid_ref, size_x):
    points = []
    for k in range(GROUP):
        offsets = offsets_ref[k : k + 1, :]
        mask = depth_lines(corner_ref[2, first + k], offsets, grid_ref.shape[-1])
        values = box_values(grid_ref, corner_ref, first + k, offsets, mask, size_x)
        points.append(on_points(values, interp_ref[k]))
    return jnp.concatenate(points, axis=0)


def latent_kernel(
    corner_ref,
    place_ref,
    chosen_ref,
    kern_ref,
    rows_ref,
    interp_ref,
    offsets_ref,
    latent_ref,
    image_ref,
    plane_ref,
    grid_ref,
):
    step = pl.program_id(0)
    size_x = kern_ref.shape[1]
    prepare(step, kern_ref, rows_ref, plane_ref, grid_ref)

    @pl.when(step == LOADS + MIXES)
    def _():
        own_planes(image_ref, grid_ref, place_ref[1], size_x)

    @pl.when(step >= LOADS + MIXES)
    def _():
        first = (step - LOADS - MIXES) * GROUP
        latent_ref[...] = field_points(
            first, corner_ref, offsets_ref, interp_ref, grid_ref, size_x
        )


def bend_kernel(
    corner_ref,
    place_ref,
    chosen_ref,
    kern_ref,
    rows_ref,
    interp_ref,
    offsets_ref,
    latent_ref,
    slope_ref,
    curvature_ref,
    plane_ref,
    grid_ref,
):
    step = pl.program_id(0)
    prepare(step, kern_ref, rows_ref, plane_ref, grid_ref)

    @pl.when(step >= LOADS + MIXES)
    def _():
        first = (step - LOADS - MIXES) * GROUP
        bend = field_points(
            first, corner_ref, offsets_ref, interp_ref, grid_ref, kern_ref.shape[1]
        )
        probability = 1.0 / (1.0 + jnp.exp(-(latent_ref[...] + chosen_ref[0] * slope_ref[...])))
        curvature_ref[...] = probability * (1.0 - probability) * bend


def spread_kernel(
    corner_ref,
    place_ref,
    chosen_ref,
    kern_ref,
    rows_ref,
    interp_ref,
    offsets_ref,
    labels_ref,
    latent_ref,
    slope_ref,
    turn_ref,
    own_ref,
    other_ref,
    plane_ref,
    grid_ref,
    sum_ref,
):
    step = pl.program_id(0)
    steps = pl.num_programs(0)
    size_x = sum_ref.shape[0]
    size_z = sum_ref.shape[-1]
    prepare(step, kern_ref, rows_ref, plane_ref, grid_ref)

    @pl.when(step < LOADS)
    def _():
        some = size_x // LOADS
        sum_ref[pl.ds(step * some, some)] = jnp.zeros((some, *sum_ref.shape[1:]), F32)

    @pl.when(step == LOADS + MIXES)
    def _():
        own_planes(turn_ref, grid_ref, place_ref[1], size_x)

    @pl.when((step >= LOADS + MIXES) & (step < steps - FLUSHES))
    def _():
        first = (step - LOADS - MIXES) * GROUP
        slope = field_points(first, corner_ref, offsets_ref, interp_ref, grid_ref, size_x)
        slope_ref[...] = slope
        probability = 1.0 / (1.0 + jnp.exp(-(latent_ref[...] + chosen_ref[0] * slope)))
        residual = labels_ref[...].astype(F32) - probability
        for k in range(GROUP):
            offsets = offsets_ref[k : k + 1, :]
            mask = depth_lines(corner_ref[2, first + k], offsets, size_z)
            term = jnp.dot(
                residual[k : k + 1].astype(BF16), interp_ref[k], preferred_element_type=F32
            )
            high = term.astype(BF16).astype(F32)
            low = term - high
            placed = jnp.concatenate(
                [
                    jnp.where(mask, high, 0.0).astype(BF16),
                    jnp.where(mask, low, 0.0).astype(BF16),
                ],
                axis=0,
            )
            row = lax.broadcasted_iota(I32, (BOXX * BOXY, offsets.shape[1]), 0)
            hot = jnp.where(row == offsets // BOXZ, 1.0, 0.0).astype(BF16)
            added = lax.dot_general(
                hot, placed, (((1,), (1,)), ((), ())), preferred_element_type=F32
            )
            added = (added[:, :size_z] + added[:, size_z:]).reshape(BOXX, BOXY, size_z)
            spot = (
                pl.ds(corner_ref[0, first + k], BOXX),
                pl.ds(corner_ref[1, first + k], BOXY),
                slice(None),
            )
            sum_ref[spot] = sum_ref[spot] + added

    half = FLUSHES // CORES
    for part, (out_ref, core) in enumerate(
        ((other_ref, CORES - 1 - place_ref[0]), (own_ref, place_ref[0]))
    ):
        start = steps - FLUSHES + part * half

        @pl.when((step >= start) & (step < start + half))
        def _():
            chips, slab = out_ref.shape[:2]
            for c in range(chips):
                for r in range(slab):
                    device = ((step - start) * chips + c) * CORES + core
                    out_ref[c, r] = sum_ref[device * slab + r]


def run(kernel, name, scalars, kern, rows, interp, offsets, extra, slab, size_y):
    devices = rows.shape[0]
    size_z = rows.shape[2]
    size_x = slab * devices
    blocks, points, columns = interp.shape
    groups = blocks // GROUP
    before = LOADS + MIXES
    at = lambda i: jnp.clip(i - before, 0, groups - 1)
    whole = lambda *shape: pl.BlockSpec(shape, lambda i, *_: (0,) * len(shape))
    point_spec = pl.BlockSpec((GROUP, points), lambda i, *_: (at(i), 0))
    point_shape = jax.ShapeDtypeStruct((blocks, points), F32)
    image_spec = whole(slab, size_y, size_z)
    image_shape = jax.ShapeDtypeStruct((slab, size_y, size_z), F32)
    scratch = [pltpu.VMEM((size_x * size_y, size_z), F32) for _ in range(2)]
    steps = before + groups
    if kernel is bend_kernel:
        out_specs, out_shape = point_spec, point_shape
    elif kernel is latent_kernel:
        out_specs, out_shape = [point_spec, image_spec], [point_shape, image_shape]
    else:
        half = FLUSHES // CORES
        chips = devices // CORES
        block = (chips // half, slab, size_y, size_z)
        flush = lambda part: pl.BlockSpec(
            block, lambda i, *_: (jnp.clip(i - steps - part * half, 0, half - 1), 0, 0, 0)
        )
        flushed = jax.ShapeDtypeStruct((chips, slab, size_y, size_z), F32)
        out_specs = [point_spec, image_spec, flush(1), flush(0)]
        out_shape = [point_shape, image_shape, flushed, flushed]
        scratch.append(pltpu.VMEM((size_x, size_y, size_z), F32))
    return pl.pallas_call(
        kernel,
        grid_spec=pltpu.PrefetchScalarGridSpec(
            num_scalar_prefetch=3,
            grid=(steps + (FLUSHES if kernel is spread_kernel else 0),),
            in_specs=[
                whole(*kern.shape),
                pl.BlockSpec(
                    (devices // LOADS, *rows.shape[1:]),
                    lambda i, *_: (jnp.minimum(i, LOADS - 1), 0, 0),
                ),
                pl.BlockSpec((GROUP, points, columns), lambda i, *_: (at(i), 0, 0)),
                pl.BlockSpec((GROUP, columns), lambda i, *_: (at(i), 0)),
                *[point_spec for _ in extra],
            ],
            out_specs=out_specs,
            scratch_shapes=scratch,
        ),
        out_shape=out_shape,
        name=name,
    )(*scalars, kern, rows, interp, offsets, *extra)


def body(
    grid_weights,
    direction,
    kern_x,
    kern_y,
    kern_z,
    interp,
    block_corner,
    block_offsets,
    labels,
    trial_steps,
    accept,
):
    slab, size_y, size_z = grid_weights.shape
    devices = lax.axis_size(PTS)
    points = interp.shape[0] * interp.shape[1] * devices
    chosen = jnp.sum(jnp.where(jnp.arange(NTRIAL) == accept[0], trial_steps, 0.0))
    core = lax.axis_index("pts_1")
    kern = jnp.concatenate(pieces_of(kern_x), axis=0)
    scalars = (block_corner, jnp.stack([core, lax.axis_index(PTS)]), chosen[None])
    common = (interp, block_offsets)

    def gathered(field, more=()):
        planes = plane_mix(field, kern_y, kern_z).reshape(slab * size_y, size_z)
        return lax.all_gather(jnp.concatenate([planes, *more], axis=0), PTS, axis=0)

    weight_rows = gathered(grid_weights)
    turn_rows = gathered(direction)
    latent, image = run(
        latent_kernel, "latent", scalars, kern, weight_rows, *common, (), slab, size_y
    )
    slope_pt, turn, own, other = run(
        spread_kernel, "spread", scalars, kern, turn_rows, *common, (labels, latent), slab, size_y
    )
    swap = [(c, CORES - 1 - c) for c in range(CORES)]
    part = (own + lax.ppermute(other, "pts_1", swap)).astype(BF16)
    spread = lax.psum_scatter(part, "pts_0", scatter_dimension=0, tiled=True)[0].astype(F32)

    target = labels.astype(F32)
    signed = 2.0 * target - 1.0
    trial_latent = latent[None] + trial_steps[:, None, None] * slope_pt[None]
    loglik = jnp.sum(jax.nn.log_sigmoid(signed[None] * trial_latent), axis=(1, 2))
    descent = jnp.sum((target[None] - jax.nn.sigmoid(trial_latent)) * slope_pt[None], axis=(1, 2))
    quad = [
        jnp.sum(grid_weights * image),
        jnp.sum(direction * image),
        jnp.sum(direction * turn),
    ]
    local = jnp.concatenate([loglik, descent, jnp.stack(quad)])
    riding = jnp.stack(pieces_of(local))
    riding = jnp.pad(riding, ((0, 16 - riding.shape[0]), (0, size_z - riding.shape[1])))

    new_weights = grid_weights + chosen * direction
    grid_gradient = spread - new_weights
    bend_rows = gathered(grid_gradient, (riding,))
    curvature = run(
        bend_kernel, "bend", scalars, kern, bend_rows, *common, (latent, slope_pt), slab, size_y
    )

    told = bend_rows[:, slab * size_y : slab * size_y + 3, : local.shape[0]]
    sums = jnp.sum(told.astype(F32), axis=(0, 1))
    loglik = sums[:NTRIAL]
    descent = sums[NTRIAL : 2 * NTRIAL]
    quad_gu, quad_du, quad_dv = sums[2 * NTRIAL], sums[2 * NTRIAL + 1], sums[2 * NTRIAL + 2]
    prior = 0.5 * (quad_gu + 2.0 * trial_steps * quad_du + trial_steps * trial_steps * quad_dv)
    trial_objective = (loglik - prior) / points
    trial_slope = (descent - quad_du - trial_steps * quad_dv) / points
    return (new_weights, grid_gradient, curvature, trial_objective, trial_slope)


def solution(mesh):
    parts = mesh.shape["parts"]
    finer = Mesh(mesh.devices.reshape(parts, -1, CORES), ("parts", "pts_0", "pts_1"))
    placed = (
        P(PARTS_PTS, None, None),
        P(PARTS_PTS, None, None),
        P(),
        P(),
        P(),
        P(PARTS_PTS, None, None),
        P(None, PARTS_PTS),
        P(PARTS_PTS, None),
        P(PARTS_PTS, None),
        P(),
        P(),
    )
    return jax.shard_map(
        body,
        mesh=finer,
        in_specs=placed,
        out_specs=(
            P(PARTS_PTS, None, None),
            P(PARTS_PTS, None, None),
            P(PARTS_PTS, None),
            P("parts"),
            P("parts"),
        ),
        check_vma=False,
    )
```
